32 devices in a mesh: expert: 8 (over y, x, core), dp: 4 (over z).
Axes of the slice: x: 2, y: 2, z: 4, core: 2. Of those that a mesh axis runs over, the one named last changes fastest.
Arguments:
- tokens: bfloat16 [256, 4096], P(('expert', 'dp')), may hold values from -6 to 6
- expert_ids: int32 [256, 2], P(('expert', 'dp')), may hold values from 0 to 7, all different within a row; in each aligned block of 8 rows (0 to 7, 8 to 15, ...) at most 4 rows name the same one
- gate_q: int32 [256, 2], P(('expert', 'dp')), may hold values from 1 to 255
- capacity: int32 [8], replicated, may hold values from 2 to 4, as said below
- w_gate: bfloat16 [8, 4096, 14336], P('dp', None, 'expert'), may hold values from -0.09375 to 0.09375
- w_up: bfloat16 [8, 4096, 14336], P('dp', None, 'expert'), may hold values from -0.09375 to 0.09375
- w_down: bfloat16 [8, 14336, 4096], P('dp', 'expert'), may hold values from -0.046875 to 0.046875
Outputs:
- mixed: bfloat16 [256, 4096], P(('expert', 'dp'))
The draws below stay inside these ranges and needn't reach their ends.
Inputs may be any that keep to these rules, and one draw needn't show every extreme that they name: `expert_ids`: each token names two different experts; among the tokens of one device no expert is named more than 4 times. `capacity`: at least half of the experts have exactly 4.
All inputs are finite; a program needn't handle non-finite values.
Results may differ from the reference program's by a relative error of at most 0.005.
Values may be sent and summed in bfloat16 or wider, within the bound.
A program may use at most 192 MiB of HBM per device.

```python
import math
import jax
import jax.numpy as jnp
import numpy as np
from jax import lax

D = 4096
FF = 14336
EXPERTS = 8
TOK_DEV = 8
CAP = 4
TOKENS = 256


def draw_capacity(key, part):
    folded = jax.random.fold_in(key, 11)
    low_key, pick_key = jax.random.split(folded)
    lowered = jax.random.randint(low_key, (EXPERTS,), 2, CAP + 1)
    order = jax.random.permutation(pick_key, EXPERTS)
    return jnp.where(order < EXPERTS // 2, CAP, lowered).astype(jnp.int32)


def touch_ends(values, stream_key, least, top_value):
    shape = values.shape
    place = [jax.random.randint(jax.random.fold_in(stream_key, axis), (), 0, shape[axis]) for axis in range(len(shape))]
    values = values.at[tuple(place)].set(least)
    longest = shape.index(max(shape))
    place[longest] = (place[longest] + 1) % shape[longest]
    return values.at[tuple(place)].set(top_value)


def block_scale(stream_key, extent, cuts, smallest, high):
    loudness = 1.0
    for position, parts in cuts:
        heights = jax.random.uniform(jax.random.fold_in(jax.random.fold_in(stream_key, 6), position), (parts,), jnp.float32, smallest / len(cuts), high / len(cuts))
        loudness = loudness * jnp.repeat(jnp.exp(heights), extent[position] // parts).reshape((-1,) + (1,) * (len(extent) - 1 - position))
    return loudness


def deal_out(key, own, number, rows, amount, top, most, slope):
    sequence = jax.random.permutation(key, amount)
    crowded, usual = load_shares(amount, rows * top, most, slope, True), load_shares(amount, rows * top, most, slope, False)
    places = jnp.arange(amount)

    def named(sizes, offset_by):
        used = int((sizes > 0).sum())
        fixed = max(1, used // 4)
        passed = fixed + (places - fixed + offset_by * (used - fixed)) % max(1, amount - fixed)
        return jnp.zeros((amount,), jnp.int32).at[sequence[jnp.where(places < fixed, places, passed)]].set(jnp.asarray(sizes, jnp.int32))

    sizes = jnp.where(number % 4 == 0, named(crowded, number // 4), named(usual, number - number // 4 - 1))
    mixed = jax.random.permutation(jax.random.fold_in(own, 3), amount)
    giver, receiver = mixed[0:amount // 2 * 2:2], mixed[1:amount // 2 * 2:2]
    slack = jnp.minimum(sizes[giver] - 1, most - sizes[receiver]) // 2
    slack = jnp.where((giver == sequence[0]) | (receiver == sequence[0]) | (sizes[receiver] == 0), 0, jnp.maximum(slack, 0))
    passed = jax.random.randint(jax.random.fold_in(own, 4), (amount // 2,), 0, 1 << 20) % (slack + 1)
    sizes = sizes.at[giver].add(-passed).at[receiver].add(passed)
    labels = jnp.searchsorted(jnp.cumsum(sizes), jnp.arange(rows * top), side="right").astype(jnp.int32)
    listing = labels.reshape(top, rows).T
    listing = listing[jax.random.permutation(jax.random.fold_in(own, 1), rows)]
    offset_by = jax.random.randint(jax.random.fold_in(own, 2), (rows, 1), 0, top)
    return jnp.take_along_axis(listing, (jnp.arange(top)[None, :] + offset_by) % top, axis=1)


def load_shares(amount, total, limit, slope, full):
    weights = [(1 << 20) // math.isqrt(grade ** slope) + 1 for grade in range(1, amount + 1)]
    largest = limit if full else min(limit, max(-(-total // amount), total * weights[0] // sum(weights)))
    least = 1 if total - largest >= amount - 1 else 0
    counts, spare = [largest] + [least] * (amount - 1), total - largest - least * (amount - 1)
    while spare > 0:
        candidates = [i for i in range(1, amount) if counts[i] < largest] or [i for i in range(1, amount) if counts[i] < limit]
        whole, left = sum([weights[i] for i in candidates]), spare
        for i in candidates:
            more = min(limit - counts[i], max(1, left * weights[i] // whole), spare)
            counts[i] = counts[i] + more
            spare = spare - more
    return np.array(counts)


def scatter_about(rng, extent, scale, bound, cuts=(), kind=jnp.bfloat16):
    drawn = jax.random.normal(rng, extent, jnp.float32) * scale
    if len(cuts) > 0:
        drawn = block_scale(rng, extent, cuts, -0.22, 0.18) * drawn
    return jnp.clip(drawn, min=-bound, max=bound).astype(kind)


def setup_inputs(seed: int = 0) -> dict:
    seeds = jax.random.split(jax.random.key(seed), 8)
    tokens = scatter_about(seeds[0], (TOKENS, D), 1.0, 6.0, ((0, 32),))
    expert_ids_keys = jax.random.split(jax.random.fold_in(seeds[1], 1), TOKENS // TOK_DEV)
    expert_ids_turns = jax.random.permutation(jax.random.fold_in(seeds[1], 3), TOKENS // TOK_DEV)
    expert_ids = jax.vmap(lambda own, number: deal_out(jax.random.fold_in(seeds[1], 2), own, number, TOK_DEV, EXPERTS, 2, CAP, 2))(expert_ids_keys, expert_ids_turns).reshape((TOKENS, 2))
    gate_q = touch_ends(jax.random.randint(seeds[2], (TOKENS, 2), 1, 256), jax.random.fold_in(seeds[2], 1), 1, 255).astype(jnp.int32)
    capacity = draw_capacity(jax.random.fold_in(seeds[7], 71), 0)
    w_gate = scatter_about(seeds[4], (EXPERTS, D, FF), D ** -0.5, 0.09375, ((0, 4), (2, 8)))
    w_up = scatter_about(seeds[5], (EXPERTS, D, FF), D ** -0.5, 0.09375, ((0, 4), (2, 8)))
    w_down = scatter_about(seeds[6], (EXPERTS, FF, D), FF ** -0.5, 0.046875, ((0, 4), (1, 8)))
    return dict(tokens=tokens, expert_ids=expert_ids, gate_q=gate_q, capacity=capacity, w_gate=w_gate, w_up=w_up, w_down=w_down)


def slot_table(expert_ids, capacity):
    flat_ids = expert_ids.reshape(-1)
    matches = (flat_ids[:, None] == jnp.arange(EXPERTS, dtype=jnp.int32)[None, :]).astype(jnp.int32)
    before = jnp.cumsum(matches, axis=0) - matches
    rank_in = jnp.sum(before * matches, axis=1)
    limit_of = jnp.sum(matches * capacity[None, :], axis=1)
    slot_of = flat_ids * CAP + rank_in
    chosen = slot_of[None, :] == jnp.arange(EXPERTS * CAP, dtype=jnp.int32)[:, None]
    return chosen & (rank_in < limit_of)[None, :]


def mixing(gate_q):
    levels = gate_q.astype(jnp.float32)
    return (levels / jnp.sum(levels, axis=1, keepdims=True)).reshape(-1)


def expert_block(operands):
    slot_rows, gate_mat, up_mat, down_mat = operands
    gate_val = jnp.dot(slot_rows, gate_mat, preferred_element_type=jnp.float32)
    up_value = jnp.dot(slot_rows, up_mat, preferred_element_type=jnp.float32)
    hidden = (jax.nn.silu(gate_val) * up_value).astype(jnp.bfloat16)
    return jnp.dot(hidden, down_mat, preferred_element_type=jnp.float32)


def reference(tokens, expert_ids, gate_q, capacity, w_gate, w_up, w_down):
    blocks = TOKENS // TOK_DEV
    token_blocks = tokens.reshape(blocks, TOK_DEV, D)
    tables = jax.vmap(slot_table, in_axes=(0, None))(expert_ids.reshape(blocks, TOK_DEV, 2), capacity)
    mixes = jax.vmap(mixing)(gate_q.reshape(blocks, TOK_DEV, 2))
    picker = tables.reshape(blocks, EXPERTS * CAP, TOK_DEV, 2).sum(axis=3).astype(jnp.float32)
    slot_rows = jnp.einsum("bst,btd->bsd", picker, token_blocks.astype(jnp.float32),
                           precision=lax.Precision.HIGHEST).astype(jnp.bfloat16)
    per_expert = slot_rows.reshape(blocks, EXPERTS, CAP, D).transpose(1, 0, 2, 3).reshape(EXPERTS, blocks * CAP, D)
    outputs = lax.map(expert_block, (per_expert, w_gate, w_up, w_down))
    outputs = outputs.reshape(EXPERTS, blocks, CAP, D).transpose(1, 0, 2, 3).reshape(blocks, EXPERTS * CAP, D)
    combine = tables.astype(jnp.float32) * mixes[:, None, :]
    spread = jnp.einsum("bsa,bsd->bad", combine, outputs, precision=lax.Precision.HIGHEST)
    mixed = spread.reshape(blocks, TOK_DEV, 2, D).sum(axis=2)
    return mixed.reshape(TOKENS, D).astype(jnp.bfloat16)
```

```python
import functools
import jax
import jax.numpy as jnp
from jax import lax
from jax.experimental import pallas as pl
from jax.experimental.pallas import tpu as pltpu
from jax.sharding import PartitionSpec as P

CAP = 4


def flip(index, bits):
    bit = 1
    while bit <= bits:
        if bits & bit:
            index = index + bit * (1 - 2 * ((index // bit) % 2))
        bit *= 2
    return index


def upper_bits(size):
    bits, bit = [], 2
    while bit < size:
        bits.append(bit)
        bit *= 2
    return bits


def to(expert, dp):
    return {"expert": expert, "dp": dp}


def remote(src, dst, send, recv, target):
    return pltpu.make_async_remote_copy(
        src_ref=src, dst_ref=dst, send_sem=send, recv_sem=recv,
        device_id=target, device_id_type=pl.DeviceIdType.MESH,
    )


def greet(members, groups, me, group):
    barrier = pltpu.get_barrier_semaphore()
    bits = [1] + upper_bits(members)
    for bit in bits:
        pl.semaphore_signal(barrier, inc=1, device_id=to(flip(me, bit), group),
                            device_id_type=pl.DeviceIdType.MESH)
    for step in range(1, groups):
        pl.semaphore_signal(barrier, inc=1, device_id=to(me, lax.rem(group + step, groups)),
                            device_id_type=pl.DeviceIdType.MESH)
    pl.semaphore_wait(barrier, len(bits) + groups - 1)


def gather_kernel(members, groups, slots_ref, all_ref, dp_send, dp_recv, send, recv, own_sem):
    me = lax.axis_index("expert")
    group = lax.axis_index("dp")
    greet(members, groups, me, group)
    own = pltpu.make_async_copy(slots_ref.at[group], all_ref.at[me, group], own_sem)
    own.start()
    sent = []
    for step in range(1, groups):
        other = lax.rem(group + step, groups)
        copy = remote(slots_ref.at[other], all_ref.at[me, group], dp_send.at[step], dp_recv.at[step],
                      to(me, other))
        copy.start()
        sent.append(copy)
    own.wait()
    for copy in sent:
        copy.wait_recv()

    half = groups // 2
    bits = upper_bits(members)
    orders = (bits[::-1], bits)

    def pass_on(side, offset, bit):
        entry = all_ref.at[flip(me, offset), pl.ds(side * half, half)]
        arriving = offset ^ bit
        copy = remote(entry, entry, send.at[side, arriving], recv.at[side, arriving],
                      to(flip(me, bit), group))
        copy.start()
        sent.append(copy)
        return copy

    held = ([0], [0])
    crossing = []
    for stage in range(len(bits)):
        started = []
        for side in range(2):
            bit = orders[side][stage]
            started.append([(offset ^ bit, pass_on(side, offset, bit)) for offset in held[side]])
        if stage == 0:
            for side in range(2):
                crossing.append(pass_on(side, 0, 1))
        fresh = []
        for side in range(2):
            for offset, copy in started[side]:
                copy.wait_recv()
                held[side].append(offset)
                fresh.append((side, offset))
        if stage + 1 == len(bits):
            for side, offset in fresh:
                crossing.append(pass_on(side, offset, 1))
        else:
            pending = fresh
            later = [(side, offset) for side, offset in pending]
            for side, offset in later:
                crossing.append(pass_on(side, offset, 1))
    for copy in crossing:
        copy.wait_recv()
    for copy in sent:
        copy.wait_send()


def reduce_kernel(members, groups, part_ref, out_ref, near, *scratch):
    bits = upper_bits(members)
    stages = len(bits)
    sums = (scratch[0:stages + 1], scratch[stages + 1:2 * stages + 2])
    rest = scratch[2 * stages + 2:]
    lands = (rest[0:stages], rest[stages:2 * stages])
    near_send, near_recv, send, recv, dp_send, dp_recv, own_sem = rest[2 * stages:]
    me = lax.axis_index("expert")
    group = lax.axis_index("dp")
    core = me % 2
    half = groups // 2
    greet(members, groups, me, group)
    cross = remote(part_ref.at[:, 1 - core], near, near_send, near_recv, to(flip(me, 1), group))
    cross.start()
    cross.wait_recv()
    orders = (bits, bits[::-1])
    f32 = jnp.float32

    def entry(ref, side, count, part, k):
        return ref.at[k, part] if side == 0 else ref.at[part, k]

    def first_sum(side, part):
        count = members // 4
        for k in range(count):
            index = 2 * k + part if side == 0 else part * count + k
            rows = pl.ds(side * half, half)
            total = part_ref[index, core, rows].astype(f32) + near[index, rows].astype(f32)
            entry(sums[side][0], side, count, part, k)[...] = total.astype(jnp.bfloat16)

    def next_sum(side, stage, mine, part):
        count = members >> (stage + 2)
        arrived = lands[side][stage - 1]
        for k in range(count):
            index = 2 * k + part if side == 0 else part * count + k
            before = entry(sums[side][stage - 1], side, 2 * count, mine, index)
            total = before[...].astype(f32) + arrived[index].astype(f32)
            entry(sums[side][stage], side, count, part, k)[...] = total.astype(jnp.bfloat16)

    def mine_of(side, stage):
        return (me // orders[side][stage]) % 2

    copies = []

    def launch(side, stage):
        other = 1 - mine_of(side, stage)
        source = sums[side][stage]
        source = source.at[:, other] if side == 0 else source.at[other]
        copy = remote(source, lands[side][stage], send.at[side, stage], recv.at[side, stage],
                      to(flip(me, orders[side][stage]), group))
        copy.start()
        copies.append(copy)
        return copy

    flying = [None, None]
    for side in range(2):
        first_sum(side, 1 - mine_of(side, 0))
        flying[side] = launch(side, 0)
    for side in range(2):
        first_sum(side, mine_of(side, 0))
    for stage in range(1, stages):
        after = [None, None]
        for side in range(2):
            flying[side].wait_recv()
            next_sum(side, stage, mine_of(side, stage - 1), 1 - mine_of(side, stage))
            after[side] = launch(side, stage)
        for side in range(2):
            next_sum(side, stage, mine_of(side, stage - 1), mine_of(side, stage))
        flying = after
    for side in range(2):
        flying[side].wait_recv()
        last = entry(sums[side][stages - 1], side, 1, mine_of(side, stages - 1), 0)
        total = last[...].astype(f32) + lands[side][stages - 1][0].astype(f32)
        scratch_final = sums[0][stages]
        scratch_final[pl.ds(side * half, half)] = total.astype(jnp.bfloat16)
    final = sums[0][stages]
    backs = []
    for step in range(1, groups):
        other = lax.rem(group + step, groups)
        copy = remote(final.at[other], out_ref.at[group], dp_send.at[step], dp_recv.at[step],
                      to(me, other))
        copy.start()
        backs.append(copy)
    own = pltpu.make_async_copy(final.at[group], out_ref.at[group], own_sem)
    own.start()
    own.wait()
    for copy in backs:
        copy.wait()
    for copy in copies:
        copy.wait_send()
    cross.wait_send()


def gather_slots(slots, members):
    groups, rows, width = slots.shape
    dma = pltpu.SemaphoreType.DMA
    return pl.pallas_call(
        functools.partial(gather_kernel, members, groups),
        out_shape=jax.ShapeDtypeStruct((members,) + slots.shape, slots.dtype),
        in_specs=[pl.BlockSpec(memory_space=pltpu.VMEM)],
        out_specs=pl.BlockSpec(memory_space=pltpu.VMEM),
        scratch_shapes=[dma((groups,)), dma((groups,)), dma((2, members)), dma((2, members)), dma],
        compiler_params=pltpu.CompilerParams(collective_id=0, has_side_effects=True),
    )(slots)


def reduce_parts(parts):
    members, groups, rows, width = parts.shape
    half = groups // 2
    kind = parts.dtype
    bits = upper_bits(members)
    block = (half, rows, width)
    left, right, left_land, right_land = [], [], [], []
    for stage in range(len(bits)):
        count = members >> (stage + 2)
        left.append(pltpu.VMEM((count, 2) + block, kind))
        right.append(pltpu.VMEM((2, count) + block, kind))
        left_land.append(pltpu.VMEM((count,) + block, kind))
        right_land.append(pltpu.VMEM((count,) + block, kind))
    left.append(pltpu.VMEM((groups, rows, width), kind))
    right.append(pltpu.VMEM((8, 128), kind))
    dma = pltpu.SemaphoreType.DMA
    return pl.pallas_call(
        functools.partial(reduce_kernel, members, groups),
        out_shape=jax.ShapeDtypeStruct((groups, rows, width), kind),
        in_specs=[pl.BlockSpec(memory_space=pltpu.VMEM)],
        out_specs=pl.BlockSpec(memory_space=pltpu.VMEM),
        scratch_shapes=[pltpu.VMEM((members // 2, groups, rows, width), kind)]
        + left + right + left_land + right_land
        + [dma, dma, dma((2, len(bits))), dma((2, len(bits))), dma((groups,)), dma((groups,)), dma],
        compiler_params=pltpu.CompilerParams(collective_id=1, has_side_effects=True),
    )(parts.reshape(members // 2, 2, groups, rows, width))


def slot_table(expert_ids, capacity):
    experts = capacity.shape[0]
    flat_ids = expert_ids.reshape(-1)
    matches = (flat_ids[:, None] == jnp.arange(experts, dtype=jnp.int32)[None, :]).astype(jnp.int32)
    before = jnp.cumsum(matches, axis=0) - matches
    rank_in = jnp.sum(before * matches, axis=1)
    limit_of = jnp.sum(matches * capacity[None, :], axis=1)
    slot_of = flat_ids * CAP + rank_in
    chosen = slot_of[None, :] == jnp.arange(experts * CAP, dtype=jnp.int32)[:, None]
    return chosen & (rank_in < limit_of)[None, :]


def per_device(tokens, expert_ids, gate_q, capacity, w_gate, w_up, w_down):
    local_experts = w_gate.shape[0]
    experts = capacity.shape[0]
    width = tokens.shape[1]
    groups = lax.axis_size("dp")
    members = lax.axis_size("expert")
    own_table = slot_table(expert_ids, capacity)
    levels = gate_q.astype(jnp.float32)
    mixes = (levels / jnp.sum(levels, axis=1, keepdims=True)).reshape(-1)
    picker = own_table.reshape(experts * CAP, -1, 2).sum(axis=2).astype(jnp.bfloat16)
    slot_rows = jnp.dot(picker, tokens, preferred_element_type=jnp.float32).astype(jnp.bfloat16)
    slot_rows = slot_rows.reshape(groups, local_experts * CAP, width)
    arrived = gather_slots(slot_rows, members)
    blocks = arrived.reshape(members * groups, local_experts, CAP, width)
    products = []
    for member in range(local_experts):
        row_block = blocks[:, member].reshape(-1, width)
        gate_val = jnp.dot(row_block, w_gate[member], preferred_element_type=jnp.float32)
        up_value = jnp.dot(row_block, w_up[member], preferred_element_type=jnp.float32)
        hidden = (jax.nn.silu(gate_val) * up_value).astype(jnp.bfloat16)
        product = jnp.dot(hidden, w_down[member], preferred_element_type=jnp.float32)
        products.append(product.astype(jnp.bfloat16).reshape(members, groups, CAP, width))
    parts = jnp.concatenate(products, axis=2)
    returned = reduce_parts(parts).reshape(experts * CAP, width)
    combine = own_table.astype(jnp.float32) * mixes[None, :]
    by_token = combine.reshape(experts * CAP, -1, 2).sum(axis=2)
    mixed = jnp.einsum("st,sd->td", by_token, returned.astype(jnp.float32),
                       precision=lax.Precision.HIGHEST)
    return mixed.astype(jnp.bfloat16)


def solution(mesh):
    in_specs = (
        P(("expert", "dp"), None),
        P(("expert", "dp"), None),
        P(("expert", "dp"), None),
        P(),
        P("dp", None, "expert"),
        P("dp", None, "expert"),
        P("dp", "expert", None),
    )
    out_specs = P(("expert", "dp"), None)
    return jax.shard_map(
        per_device, mesh=mesh, in_specs=in_specs, out_specs=out_specs, check_vma=False
    )
```
